256 devices in a mesh: qa: 32 (over z, x_lo, core), qb: 8 (over y, x_hi).
Axes of the slice: x: 4 (x_hi: 2, x_lo: 2; x = x_hi * 2 + x_lo), y: 4, z: 8, core: 2. Of those that a mesh axis runs over, the one named last changes fastest.
Arguments:
- wave_parts: float32 [2, 2048, 128, 128], P(None, ('qa', 'qb')), may hold values from -6 to 6
- level_table: float32 [2048, 128, 128], P(('qa', 'qb')), may hold values from -2 to 2
- phase_angles: float32 [2, 128], replicated, may hold values from 0.3 to 1.2
Outputs:
- final_parts: float32 [2, 2048, 128, 128], P(None, ('qa', 'qb'))
The draws below stay inside these ranges and needn't reach their ends.
All inputs are finite; a program needn't handle non-finite values.
Results may differ from the reference program's by a relative error of at most 0.0003.
Values sent between devices are 32-bit elements; how exact they have to be, the bound alone decides.
A program may use at most 64 MiB of HBM per device.

```python
import jax
import jax.numpy as jnp
from jax import lax

BLOCKS_DEV = 8
ROWS = 128
LANES = 128
BLOCKS = 2048
LAYERS = 2
N_QA = 32
N_QB = 8


def shard_levels(stream_key, dims, cuts, low, top_value):
    def one(position, blocks):
        heights = jax.random.uniform(jax.random.fold_in(jax.random.fold_in(stream_key, 6), position), (blocks,), jnp.float32, low / len(cuts), top_value / len(cuts))
        return jnp.repeat(jnp.exp(heights), dims[position] // blocks).reshape((-1,) + (1,) * (len(dims) - position - 1))

    gain = one(*cuts[0])
    for cut in cuts[1:]:
        gain = gain * one(*cut)
    return gain


def bell_draw(key, dims, width, most, pieces=(), kind=jnp.bfloat16):
    level = shard_levels(key, dims, pieces, -0.22, 0.18) if pieces else 1.0
    result = jax.random.normal(key, dims, jnp.float32) * width * level
    return jnp.minimum(jnp.maximum(result, -most), most).astype(kind)


def setup_inputs(seed: int = 0) -> dict:
    seeds = jax.random.split(jax.random.key(seed), 4)
    wave_parts = bell_draw(seeds[0], (2, BLOCKS, ROWS, LANES), 1.0, 6.0, ((1, 256),), jnp.float32)
    level_table = jnp.clip(jax.random.uniform(seeds[1], (BLOCKS, ROWS, LANES), jnp.float32, -2.0, 2.0) * shard_levels(seeds[1], (BLOCKS, ROWS, LANES), ((0, 256),), -0.4, 0.0), -2.0, 2.0)
    phase_angles = jnp.clip(jax.random.uniform(seeds[2], (LAYERS, LANES), jnp.float32, 0.3, 1.2), 0.3, 1.2)
    return {"wave_parts": wave_parts, "level_table": level_table, "phase_angles": phase_angles}


def count_bits(values, count):
    places = jnp.arange(count.bit_length() - 1, dtype=jnp.int32)
    return jnp.sum((values[..., None] >> places) & 1, axis=-1)


def sign_table(count):
    rank = jnp.arange(count, dtype=jnp.int32)
    parity = count_bits(rank[:, None] & rank[None, :], count) % 2
    real_part = jnp.where(parity == 1, -1.0, 1.0).astype(jnp.float32) * (count ** -0.5)
    return real_part


def turn_dim(values, dim):
    real_part = sign_table(values.shape[dim])
    def times(table):
        moved = jnp.tensordot(values, table, axes=([dim], [0]), precision=lax.Precision.HIGHEST)
        return jnp.moveaxis(moved, -1, dim)
    return times(real_part)


def turn_phase(values, levels, angle):
    turn = angle * levels
    return jnp.stack([values[0] * jnp.cos(turn) + values[1] * jnp.sin(turn), values[1] * jnp.cos(turn) - values[0] * jnp.sin(turn)])


def reference(wave_parts, level_table, phase_angles):
    values = wave_parts
    for layer in range(LAYERS):
        values = turn_phase(values, level_table, phase_angles[layer])
        values = turn_dim(values, 3)
        values = turn_dim(values, 2)
        parts = values.reshape(2, N_QA, N_QB, BLOCKS_DEV, ROWS, LANES)
        parts = turn_dim(parts, 1)
        parts = turn_dim(parts, 2)
        parts = turn_dim(parts, 3)
        values = parts.reshape(values.shape)
    return values
```

```python
import functools

import jax
import jax.numpy as jnp
from jax import lax
from jax.experimental import pallas as pl
from jax.experimental.pallas import tpu as pltpu
from jax.sharding import PartitionSpec as P

MESH = pl.DeviceIdType.MESH
SCALE = 2.0**-12.5
CHIPS = 128


def place():
    qa, qb = lax.axis_index("qa"), lax.axis_index("qb")
    return qa // 4, (qa // 2) % 2 * 8 + qb, qa % 2


def device(z, w, core):
    return (z * 4 + w // 8 * 2 + core, w % 8)


def plane_step(w, d):
    xlo = (w // 8 + d // 8) % 2
    y = (w // 2 % 4 + d // 2 % 4) % 4
    xhi = (w % 2 + d % 2) % 2
    return xlo * 8 + y * 2 + xhi


def fwht(tiles):
    tiles = list(tiles)
    step = 1
    while step < len(tiles):
        for i in range(len(tiles)):
            if not i & step:
                u, v = tiles[i], tiles[i + step]
                tiles[i], tiles[i + step] = u + v, u - v
        step *= 2
    return tiles


def sign_matrix(count):
    both = lax.broadcasted_iota(jnp.int32, (count, count), 0) & lax.broadcasted_iota(jnp.int32, (count, count), 1)
    for shift in (4, 2, 1):
        both = both ^ (both >> shift)
    return (1 - 2 * (both & 1)).astype(jnp.float32).astype(jnp.bfloat16)


def halves(x):
    high = x.astype(jnp.bfloat16)
    return high, (x - high.astype(jnp.float32)).astype(jnp.bfloat16)


def turn_lanes(x, signs):
    high, low = halves(x)
    dot = functools.partial(jnp.dot, preferred_element_type=jnp.float32)
    return dot(high, signs) + dot(low, signs)


def turn_rows(x, signs):
    high, low = halves(x)
    dot = functools.partial(jnp.dot, preferred_element_type=jnp.float32)
    return dot(signs, high) + dot(signs, low)


def kernel(
    wave_ref, level_ref, angle_ref, out_ref,
    wave, level, local, local_in, send, recv, level_in, cos2, sin2, mix, mix_in, back, back_in, final,
    in_sem, out_sem, pair_send, pair_recv, level_send, level_recv, there_send, there_recv, back_send, back_recv, ready,
):
    z, w, core = place()
    me = z * 16 + w
    partner = device(z, w, 1 - core)
    own_sign = (1 - 2 * core).astype(jnp.float32)

    barrier = pltpu.get_barrier_semaphore()

    def signal(sem, to):
        pl.semaphore_signal(sem, inc=1, device_id=to, device_id_type=MESH)

    @pl.loop(1, 8)
    def _(d):
        signal(barrier, device((z + d) % 8, w, core))

    @pl.loop(1, 16)
    def _(d):
        signal(barrier, device(z, plane_step(w, d), core))

    signal(barrier, partner)

    level_copy = pltpu.make_async_copy(level_ref, level, in_sem.at[0])
    wave_copy = pltpu.make_async_copy(wave_ref, wave, in_sem.at[1])
    level_copy.start()
    wave_copy.start()
    signs = sign_matrix(128)
    level_copy.wait()

    pl.semaphore_wait(barrier, 23)

    @pl.loop(1, 16)
    def _(d):
        signal(ready, device(z, plane_step(w, d), core))

    pl.semaphore_wait(ready, 15)

    def peer(m):
        d = m % 8 * 16 + m // 8
        return (z + d // 16) % 8, plane_step(w, d % 16)

    @pl.loop(1, CHIPS)
    def _(m):
        pz, pw = peer(m)
        pltpu.make_async_remote_copy(
            level.at[pz, pl.ds(pw * 8, 8)], level_in.at[me], level_send, level_recv,
            device_id=device(pz, pw, core), device_id_type=MESH,
        ).start()

    wave_copy.wait()

    @pl.loop(0, 8)
    def _(b):
        turn = angle_ref[0:1] * level[b]
        c, s = jnp.cos(turn) * SCALE, jnp.sin(turn) * SCALE
        re, im = wave[0, b], wave[1, b]
        for part, x in enumerate((re * c + im * s, im * c - re * s)):
            local[part, b] = turn_rows(turn_lanes(x, signs), signs)

    @pl.loop(0, 16)
    def _(t):
        rows = pl.ds(t * 8, 8)
        for part in range(2):
            for b, x in enumerate(fwht([local[part, b, rows] for b in range(8)])):
                local[part, b, rows] = x

    swap = pltpu.make_async_remote_copy(
        local, local_in, pair_send.at[0], pair_recv.at[0], device_id=partner, device_id_type=MESH
    )
    swap.start()
    swap.wait()

    lower = lax.broadcasted_iota(jnp.int32, (8, 128), 0) < 4

    @pl.loop(0, 8)
    def _(b):
        for t in range(16):
            rows = pl.ds(t * 8, 8)
            re, im = (local_in[part, b, rows] + own_sign * local[part, b, rows] for part in range(2))
            send[0, b * 16 + t] = jnp.where(lower, re, pltpu.roll(im, 4, 0))
            send[1, b * 16 + t] = jnp.where(lower, pltpu.roll(re, 4, 0), im)

    def spread(src, dst, send_sem, recv_sem):
        @pl.loop(1, CHIPS)
        def _(m):
            pz, pw = peer(m)
            pltpu.make_async_remote_copy(
                src.at[pz * 16 + pw], dst.at[me], send_sem, recv_sem,
                device_id=device(pz, pw, core), device_id_type=MESH,
            ).start()

    def gathered(src, dst, send_sem, recv_sem):
        return pltpu.make_async_remote_copy(
            src.at[pl.ds(0, CHIPS - 1)], dst.at[pl.ds(0, CHIPS - 1)], send_sem, recv_sem,
            device_id=partner, device_id_type=MESH,
        )

    for k in range(2):
        spread(send.at[k], recv.at[k], there_send.at[k], there_recv.at[k])
        recv[k, me] = send[k, me]
    level_in[me] = level[z, pl.ds(w * 8, 8)]

    gathered(level_in, level_in, level_send, level_recv).wait_recv()

    @pl.loop(0, CHIPS)
    def _(t):
        turn = angle_ref[1:2] * level_in[t]
        cos2[t] = jnp.cos(turn) * SCALE
        sin2[t] = jnp.sin(turn) * SCALE

    sublane = lax.broadcasted_iota(jnp.int32, (8, 128), 0)

    def turn_sublanes(x, step):
        upper = (sublane & step) != 0
        other = jnp.where(upper, pltpu.roll(x, step, 0), pltpu.roll(x, 8 - step, 0))
        return other + jnp.where(upper, -x, x)

    for k in range(2):
        gathered(send.at[k], recv.at[k], there_send.at[k], there_recv.at[k]).wait_recv()

        @pl.loop(0, 8)
        def _(i):
            for j, x in enumerate(fwht([recv[k, i * 16 + j] for j in range(16)])):
                recv[k, i * 16 + j] = x

        @pl.loop(0, 16)
        def _(j):
            tiles = fwht([recv[k, i * 16 + j] for i in range(8)])
            for i in range(8):
                c, s = cos2[i * 16 + j], sin2[i * 16 + j]
                if k == 0:
                    c, s = jnp.where(lower, c, pltpu.roll(c, 4, 0)), jnp.where(lower, s, -pltpu.roll(s, 4, 0))
                else:
                    c, s = jnp.where(lower, pltpu.roll(c, 4, 0), c), jnp.where(lower, pltpu.roll(s, 4, 0), -s)
                tiles[i] = tiles[i] * c + pltpu.roll(tiles[i], 4, 0) * s
            for i, x in enumerate(fwht(tiles)):
                recv[k, i * 16 + j] = x

        @pl.loop(0, 8)
        def _(i):
            tiles = fwht([recv[k, i * 16 + j] for j in range(16)])
            tiles = [turn_sublanes(turn_sublanes(x, 1), 2) for x in tiles]
            x = turn_lanes(jnp.concatenate(tiles, axis=0), signs)
            for j in range(16):
                mix[k, i * 16 + j] = x[j * 8 : j * 8 + 8]

        swap = pltpu.make_async_remote_copy(
            mix.at[k], mix_in.at[k], pair_send.at[1 + k], pair_recv.at[1 + k], device_id=partner, device_id_type=MESH
        )
        swap.start()
        swap.wait()

        @pl.loop(0, 8)
        def _(i):
            for j in range(16):
                t = i * 16 + j
                back[k, t] = mix_in[k, t] + own_sign * mix[k, t]

        spread(back.at[k], back_in.at[k], back_send.at[k], back_recv.at[k])
        back_in[k, me] = back[k, me]

    for k in range(2):
        gathered(back.at[k], back_in.at[k], back_send.at[k], back_recv.at[k]).wait_recv()

        @pl.loop(0, 8)
        def _(i):
            for j, x in enumerate(fwht([back_in[k, i * 16 + j] for j in range(16)])):
                back_in[k, i * 16 + j] = x

    @pl.loop(0, 16)
    def _(j):
        first, second = (fwht([back_in[k, i * 16 + j] for i in range(8)]) for k in range(2))
        rows = pl.ds(j * 8, 8)
        for i in range(8):
            u, v = first[i] + second[i], first[i] - second[i]
            final[0, i, rows] = jnp.where(lower, u, pltpu.roll(v, 4, 0))
            final[1, i, rows] = jnp.where(lower, pltpu.roll(u, 4, 0), v)

    out_copy = pltpu.make_async_copy(final, out_ref, out_sem)
    out_copy.start()
    gathered(level_in, level_in, level_send, level_recv).wait_send()
    for k in range(2):
        gathered(send.at[k], recv.at[k], there_send.at[k], there_recv.at[k]).wait_send()
        gathered(back.at[k], back_in.at[k], back_send.at[k], back_recv.at[k]).wait_send()
    out_copy.wait()


def body(wave_parts, level_table, phase_angles):
    f32 = jnp.float32
    state, tiles = pltpu.VMEM((2, 8, 128, 128), f32), pltpu.VMEM((2, CHIPS, 8, 128), f32)
    table = pltpu.VMEM((CHIPS, 8, 128), f32)
    dma = pltpu.SemaphoreType.DMA
    anywhere = pl.BlockSpec(memory_space=pl.ANY)
    return pl.pallas_call(
        kernel,
        out_shape=jax.ShapeDtypeStruct(wave_parts.shape, f32),
        in_specs=[anywhere, anywhere, pl.BlockSpec(memory_space=pltpu.VMEM)],
        out_specs=anywhere,
        scratch_shapes=[
            state, pltpu.VMEM((8, 128, 128), f32), state, state, tiles, tiles, table, table, table, tiles, tiles, tiles, tiles, state,
            dma((2,)), dma, dma((3,)), dma((3,)), dma, dma, dma((2,)), dma((2,)), dma((2,)), dma((2,)), pltpu.SemaphoreType.REGULAR,
        ],
        compiler_params=pltpu.CompilerParams(collective_id=0, has_side_effects=True),
    )(wave_parts, level_table, phase_angles)


def solution(mesh):
    in_specs = (P(None, ("qa", "qb"), None, None), P(("qa", "qb"), None, None), P())
    out_specs = P(None, ("qa", "qb"), None, None)
    return jax.shard_map(body, mesh=mesh, in_specs=in_specs, out_specs=out_specs, check_vma=False)
```

```python
import functools

import jax
import jax.numpy as jnp
from jax import lax
from jax.experimental import pallas as pl
from jax.experimental.pallas import tpu as pltpu
from jax.sharding import PartitionSpec as P

MESH = pl.DeviceIdType.MESH
SCALE = 2.0**-12.5
CHIPS = 128


def place():
    qa, qb = lax.axis_index("qa"), lax.axis_index("qb")
    return qa // 4, (qa // 2) % 2 * 8 + qb, qa % 2


def device(z, w, core):
    return (z * 4 + w // 8 * 2 + core, w % 8)


def plane_step(w, d):
    xlo = (w // 8 + d // 8) % 2
    y = (w // 2 % 4 + d // 2 % 4) % 4
    xhi = (w % 2 + d % 2) % 2
    return xlo * 8 + y * 2 + xhi


def fwht(tiles):
    tiles = list(tiles)
    step = 1
    while step < len(tiles):
        for i in range(len(tiles)):
            if not i & step:
                u, v = tiles[i], tiles[i + step]
                tiles[i], tiles[i + step] = u + v, u - v
        step *= 2
    return tiles


def sign_matrix(count):
    both = lax.broadcasted_iota(jnp.int32, (count, count), 0) & lax.broadcasted_iota(jnp.int32, (count, count), 1)
    for shift in (4, 2, 1):
        both = both ^ (both >> shift)
    return (1 - 2 * (both & 1)).astype(jnp.float32).astype(jnp.bfloat16)


def halves(x):
    high = x.astype(jnp.bfloat16)
    return high, (x - high.astype(jnp.float32)).astype(jnp.bfloat16)


def turn_lanes(x, signs):
    high, low = halves(x)
    dot = functools.partial(jnp.dot, preferred_element_type=jnp.float32)
    return dot(high, signs) + dot(low, signs)


def turn_rows(x, signs):
    high, low = halves(x)
    dot = functools.partial(jnp.dot, preferred_element_type=jnp.float32)
    return dot(signs, high) + dot(signs, low)


def kernel(
    wave_ref, level_ref, angle_hbm, out_ref,
    wave, level, angle_ref, cosine, sine, local, local_in, send, recv, level_mid, level_in, mix, mix_in, back, back_in,
    in_sem, pair_send, pair_recv, mid_send, mid_recv, level_send, level_recv, there_send, there_recv, back_send, back_recv, ready,
):
    z, w, core = place()
    me = z * 16 + w
    partner = device(z, w, 1 - core)
    own_sign = (1 - 2 * core).astype(jnp.float32)
    lower = lax.broadcasted_iota(jnp.int32, (8, 128), 0) < 4

    barrier = pltpu.get_barrier_semaphore()

    def signal(sem, to):
        pl.semaphore_signal(sem, inc=1, device_id=to, device_id_type=MESH)

    def send_to(src, dst, send_sem, recv_sem, to):
        return pltpu.make_async_remote_copy(src, dst, send_sem, recv_sem, device_id=to, device_id_type=MESH)

    level_copy = pltpu.make_async_copy(level_ref, level, in_sem.at[0])
    wave_copy = pltpu.make_async_copy(wave_ref, wave, in_sem.at[1])
    level_copy.start()
    angle_copy = pltpu.make_async_copy(angle_hbm, angle_ref, in_sem.at[2])
    angle_copy.start()
    wave_copy.start()

    @pl.loop(1, 8)
    def _(d):
        signal(barrier, device((z + d) % 8, w, core))

    @pl.loop(1, 16)
    def _(d):
        signal(barrier, device(z, plane_step(w, d), core))

    signal(barrier, partner)

    signs = sign_matrix(128)
    level_copy.wait()

    pl.semaphore_wait(barrier, 23)
    for d in (4, 3, 5, 2, 6, 1, 7):
        there = (z + d) % 8
        send_to(level.at[there], level_mid.at[z], mid_send, mid_recv.at[d - 1], device(there, w, core)).start()

    @pl.loop(1, 16)
    def _(d):
        signal(ready, device(z, plane_step(w, d), core))

    angle_copy.wait()
    wave_copy.wait()

    @pl.loop(0, 8)
    def _(b):
        turn = angle_ref[0:1] * level[b]
        c, s = jnp.cos(turn) * SCALE, jnp.sin(turn) * SCALE
        re, im = wave[0, b], wave[1, b]
        for part, x in enumerate((re * c + im * s, im * c - re * s)):
            local[part, b] = turn_rows(turn_lanes(x, signs), signs)

    level_mid[z] = level[z]

    def swap(q):
        rows = pl.ds(q * 32, 32)
        return send_to(
            local.at[:, :, rows], local_in.at[:, :, rows], pair_send.at[q], pair_recv.at[q], partner
        )

    for q in range(4):

        @pl.loop(q * 4, q * 4 + 4)
        def _(t):
            rows = pl.ds(t * 8, 8)
            for part in range(2):
                for b, x in enumerate(fwht([local[part, b, rows] for b in range(8)])):
                    local[part, b, rows] = x

        swap(q).start()

    for q in range(4):
        swap(q).wait_recv()

        @pl.loop(0, 8)
        def _(b):
            for t in range(q * 4, q * 4 + 4):
                rows = pl.ds(t * 8, 8)
                re, im = (local_in[part, b, rows] + own_sign * local[part, b, rows] for part in range(2))
                send[0, b * 16 + t] = jnp.where(lower, re, pltpu.roll(im, 4, 0))
                send[1, b * 16 + t] = jnp.where(lower, pltpu.roll(re, 4, 0), im)

    def spread(src, dst, send_sem, recv_sem):
        for d in (4, 3, 5, 2, 6, 1, 7, 0):

            @pl.loop(0 if d else 1, 16)
            def _(e):
                pz, pw = (z + d) % 8, plane_step(w, e)
                send_to(src.at[pz * 16 + pw], dst.at[me], send_sem, recv_sem, device(pz, pw, core)).start()

    def gathered(src, dst, send_sem, recv_sem):
        return send_to(src.at[pl.ds(0, CHIPS - 1)], dst.at[pl.ds(0, CHIPS - 1)], send_sem, recv_sem, partner)

    def there(k):
        return send.at[k], recv.at[k], there_send.at[k], there_recv.at[k]

    def again(k):
        return back.at[k], back_in.at[k], back_send.at[k], back_recv.at[k]

    pl.semaphore_wait(ready, 15)
    spread(*there(0))
    recv[0, me] = send[0, me]

    for d in (1, 7, 2, 6, 3, 5, 4):
        source = (z + d) % 8
        send_to(
            level.at[0], level_mid.at[source], mid_send, mid_recv.at[7 - d], device(source, w, core)
        ).wait_recv()

    @pl.loop(1, 16)
    def _(e):
        pw = plane_step(w, e)
        send_to(
            level_mid.at[:, pl.ds(pw * 8, 8)], level_in.at[:, w], level_send, level_recv, device(z, pw, core)
        ).start()

    level_in[:, w] = level_mid[:, pl.ds(w * 8, 8)]
    spread(*there(1))
    recv[1, me] = send[1, me]
    level_part = level_in.at[:, pl.ds(0, 15)]
    level_all = send_to(level_part, level_part, level_send, level_recv, partner)
    level_all.wait_recv()

    @pl.loop(0, 8)
    def _(i):
        turn = angle_ref[1:2] * level_in[i].reshape(128, 128)
        cosine[i] = (jnp.cos(turn) * SCALE).reshape(16, 8, 128)
        sine[i] = (jnp.sin(turn) * SCALE).reshape(16, 8, 128)

    sublane = lax.broadcasted_iota(jnp.int32, (8, 128), 0)

    def turn_sublanes(x, step):
        upper = (sublane & step) != 0
        other = jnp.where(upper, pltpu.roll(x, step, 0), pltpu.roll(x, 8 - step, 0))
        return other + jnp.where(upper, -x, x)

    for k in range(2):
        gathered(*there(k)).wait_recv()

        @pl.loop(0, 8)
        def _(i):
            for j, x in enumerate(fwht([recv[k, i * 16 + j] for j in range(16)])):
                recv[k, i * 16 + j] = x

        @pl.loop(0, 16)
        def _(j):
            tiles = fwht([recv[k, i * 16 + j] for i in range(8)])
            for i in range(8):
                c, s = cosine[i, j], sine[i, j]
                if k == 0:
                    c, s = jnp.where(lower, c, pltpu.roll(c, 4, 0)), jnp.where(lower, s, -pltpu.roll(s, 4, 0))
                else:
                    c, s = jnp.where(lower, pltpu.roll(c, 4, 0), c), jnp.where(lower, pltpu.roll(s, 4, 0), -s)
                tiles[i] = tiles[i] * c + pltpu.roll(tiles[i], 4, 0) * s
            for i, x in enumerate(fwht(tiles)):
                recv[k, i * 16 + j] = x

        @pl.loop(0, 8)
        def _(i):
            tiles = fwht([recv[k, i * 16 + j] for j in range(16)])
            tiles = [turn_sublanes(turn_sublanes(x, 1), 2) for x in tiles]
            x = turn_lanes(jnp.concatenate(tiles, axis=0), signs)
            for j in range(16):
                mix[k, i * 16 + j] = x[j * 8 : j * 8 + 8]

        pair = send_to(mix.at[k], mix_in.at[k], pair_send.at[4 + k], pair_recv.at[4 + k], partner)
        pair.start()
        pair.wait()

        @pl.loop(0, 8)
        def _(i):
            for j in range(16):
                t = i * 16 + j
                back[k, t] = mix_in[k, t] + own_sign * mix[k, t]

        spread(*again(k))
        back_in[k, me] = back[k, me]

    for q in range(4):
        swap(q).wait_send()
    for d in range(7):
        send_to(level.at[0], level_mid.at[0], mid_send, mid_recv.at[0], partner).wait_send()
    level_all.wait_send()
    for k in range(2):
        gathered(*there(k)).wait_send()

    for k in range(2):
        gathered(*again(k)).wait_recv()

        @pl.loop(0, 8)
        def _(i):
            for j, x in enumerate(fwht([back_in[k, i * 16 + j] for j in range(16)])):
                out_ref[k, i * 16 + j] = x

    for k in range(2):
        gathered(*again(k)).wait_send()


def finish(tiles_ref, out_ref, final, out_sem):
    lower = lax.broadcasted_iota(jnp.int32, (8, 128), 0) < 4
    copies = []
    for q in range(4):

        @pl.loop(q * 4, q * 4 + 4)
        def _(j):
            first, second = (fwht([tiles_ref[k, i * 16 + j] for i in range(8)]) for k in range(2))
            rows = pl.ds(j * 8, 8)
            for i in range(8):
                u, v = first[i] + second[i], first[i] - second[i]
                final[0, i, rows] = jnp.where(lower, u, pltpu.roll(v, 4, 0))
                final[1, i, rows] = jnp.where(lower, pltpu.roll(u, 4, 0), v)

        rows = pl.ds(q * 32, 32)
        copies.append(pltpu.make_async_copy(final.at[:, :, rows], out_ref.at[:, :, rows], out_sem.at[q]))
        copies[-1].start()
    for copy in copies:
        copy.wait()


def body(wave_parts, level_table, phase_angles):
    f32 = jnp.float32
    state, tiles = pltpu.VMEM((2, 8, 128, 128), f32), pltpu.VMEM((2, CHIPS, 8, 128), f32)
    table = pltpu.VMEM((8, 16, 8, 128), f32)
    blocks = pltpu.VMEM((8, 128, 128), f32)
    dma = pltpu.SemaphoreType.DMA
    anywhere, on_chip = pl.BlockSpec(memory_space=pl.ANY), pl.BlockSpec(memory_space=pltpu.VMEM)
    off_chip = pl.BlockSpec(memory_space=pltpu.HBM)
    args = [pltpu.with_memory_space_constraint(x, pltpu.HBM) for x in (wave_parts, level_table, phase_angles)]
    mixed = pl.pallas_call(
        kernel,
        out_shape=pltpu.VMEM((2, CHIPS, 8, 128), f32),
        in_specs=[off_chip] * 3,
        out_specs=on_chip,
        scratch_shapes=[
            state, blocks, pltpu.VMEM((2, 128), f32), table, table, state, state, tiles, tiles, blocks, table, tiles, tiles, tiles, tiles,
            dma((3,)), dma((6,)), dma((6,)), dma, dma((7,)), dma, dma, dma((2,)), dma((2,)), dma((2,)), dma((2,)), pltpu.SemaphoreType.REGULAR,
        ],
        compiler_params=pltpu.CompilerParams(collective_id=0, has_side_effects=True, vmem_limit_bytes=32 * 2**20),
    )(*args)
    return pl.pallas_call(
        finish,
        out_shape=jax.ShapeDtypeStruct(wave_parts.shape, f32),
        in_specs=[on_chip],
        out_specs=anywhere,
        scratch_shapes=[state, dma((4,))],
        compiler_params=pltpu.CompilerParams(vmem_limit_bytes=16 * 2**20),
    )(mixed)


def solution(mesh):
    in_specs = (P(None, ("qa", "qb"), None, None), P(("qa", "qb"), None, None), P())
    out_specs = P(None, ("qa", "qb"), None, None)
    return jax.shard_map(body, mesh=mesh, in_specs=in_specs, out_specs=out_specs, check_vma=False)
```

```python
import functools

import jax
import jax.numpy as jnp
from jax import lax
from jax.experimental import pallas as pl
from jax.experimental.pallas import tpu as pltpu
from jax.sharding import PartitionSpec as P

MESH = pl.DeviceIdType.MESH
SCALE = 2.0**-12.5
CHIPS = 128
FAR_FIRST = (5, 3, 7, 12, 13, 1, 4, 10, 11, 14, 15, 2, 6, 8, 9, 0)
COS = (0.9999999995270198, -0.49999999256864547, 0.04166664759094903, -0.0013888705067878636, 2.479313621797957e-05, -2.7357116288633015e-07, 1.850280961043466e-09)
SIN = (0.9999999957579141, -0.1666666176642379, 0.008333241511668515, -0.00019834965410918986, 2.7360914118386437e-06, -2.2205074368871847e-08)


def place():
    qa, qb = lax.axis_index("qa"), lax.axis_index("qb")
    return qa // 4, (qa // 2) % 2 * 8 + qb, qa % 2


def device(z, w, core):
    return (z * 4 + w // 8 * 2 + core, w % 8)


def plane(x, y):
    return x % 2 * 8 + y * 2 + x // 2


def plane_step(w, d):
    xlo = (w // 8 + d // 8) % 2
    y = (w // 2 % 4 + d // 2 % 4) % 4
    xhi = (w % 2 + d % 2) % 2
    return xlo * 8 + y * 2 + xhi


def fwht(tiles):
    tiles = list(tiles)
    step = 1
    while step < len(tiles):
        for i in range(len(tiles)):
            if not i & step:
                u, v = tiles[i], tiles[i + step]
                tiles[i], tiles[i + step] = u + v, u - v
        step *= 2
    return tiles


def polynomial(terms, x):
    value = terms[-1] * SCALE
    for term in terms[-2::-1]:
        value = value * x + term * SCALE
    return value


def scaled_turn(turn):
    square = turn * turn
    return polynomial(COS, square), turn * polynomial(SIN, square)


def sign_matrix(count):
    both = lax.broadcasted_iota(jnp.int32, (count, count), 0) & lax.broadcasted_iota(jnp.int32, (count, count), 1)
    for shift in (4, 2, 1):
        both = both ^ (both >> shift)
    return (1 - 2 * (both & 1)).astype(jnp.float32).astype(jnp.bfloat16)


def halves(x):
    high = x.astype(jnp.bfloat16)
    return high, (x - high.astype(jnp.float32)).astype(jnp.bfloat16)


def turn_lanes(x, signs):
    high, low = halves(x)
    dot = functools.partial(jnp.dot, preferred_element_type=jnp.float32)
    return dot(high, signs) + dot(low, signs)


def turn_rows(x, signs):
    high, low = halves(x)
    dot = functools.partial(jnp.dot, preferred_element_type=jnp.float32)
    return dot(signs, high) + dot(signs, low)


def kernel(
    wave_ref, level_ref, angle_hbm, out_ref,
    wave, level, angle_ref, cosine, sine, local, local_in, send, recv, level_mid, level_in, mix, mix_in, back, back_in,
    in_sem, pair_send, pair_recv, mid_send, mid_recv, level_send, level_recv, there_send, there_recv, back_send, back_recv, ready, beside,
):
    z, w, core = place()
    me = z * 16 + w
    partner = device(z, w, 1 - core)
    own_sign = (1 - 2 * core).astype(jnp.float32)
    lower = lax.broadcasted_iota(jnp.int32, (8, 128), 0) < 4

    barrier = pltpu.get_barrier_semaphore()

    def signal(sem, to):
        pl.semaphore_signal(sem, inc=1, device_id=to, device_id_type=MESH)

    def send_to(src, dst, send_sem, recv_sem, to):
        return pltpu.make_async_remote_copy(src, dst, send_sem, recv_sem, device_id=to, device_id_type=MESH)

    level_copy = pltpu.make_async_copy(level_ref, level, in_sem.at[0])
    wave_copy = pltpu.make_async_copy(wave_ref, wave, in_sem.at[1])
    level_copy.start()
    angle_copy = pltpu.make_async_copy(angle_hbm, angle_ref, in_sem.at[2])
    angle_copy.start()
    wave_copy.start()

    x, y = w % 2 * 2 + w // 8, w // 2 % 4
    y_both = [device(z, plane(x, (y + d) % 4), core) for d in (1, 3)]
    x_both = [device(z, plane((x + d) % 4, y), core) for d in (1, 3)]
    for to in [device((z + d) % 8, w, core) for d in (4, 3, 5, 2, 6, 1, 7)] + y_both + x_both + [partner]:
        signal(barrier, to)

    signs = sign_matrix(128)

    def send_levels(d):
        there = (z + d) % 8
        send_to(level.at[there], level_mid.at[z], mid_send, mid_recv.at[d - 1], device(there, w, core)).start()

    def first_turns(start, stop):
        @pl.loop(start, stop)
        def _(b):
            c, s = scaled_turn(angle_ref[0:1] * level[b])
            re, im = wave[0, b], wave[1, b]
            for part, value in enumerate((re * c + im * s, im * c - re * s)):
                local[part, b] = turn_rows(turn_lanes(value, signs), signs)

    pl.semaphore_wait(barrier, 12)
    level_copy.wait()
    for d in (4, 3, 5, 2, 6, 1, 7):
        send_levels(d)
    for to in y_both:
        signal(beside.at[0], to)
    angle_copy.wait()
    wave_copy.wait()
    for step in range(2):
        first_turns(step * 2, step * 2 + 2)
        pl.semaphore_wait(beside.at[step], 2)
        for to in x_both:
            signal(beside.at[step + 1], to)
    first_turns(4, 6)
    pl.semaphore_wait(beside.at[2], 2)

    @pl.loop(1, 16)
    def _(d):
        signal(ready, device(z, plane_step(w, d), core))

    first_turns(6, 8)

    level_mid[z] = level[z]

    def swap(q):
        rows = pl.ds(q * 32, 32)
        return send_to(
            local.at[:, :, rows], local_in.at[:, :, rows], pair_send.at[q], pair_recv.at[q], partner
        )

    for q in range(4):

        @pl.loop(q * 4, q * 4 + 4)
        def _(t):
            rows = pl.ds(t * 8, 8)
            for part in range(2):
                for b, x in enumerate(fwht([local[part, b, rows] for b in range(8)])):
                    local[part, b, rows] = x

        swap(q).start()

    for q in range(4):
        swap(q).wait_recv()

        @pl.loop(0, 8)
        def _(b):
            for t in range(q * 4, q * 4 + 4):
                rows = pl.ds(t * 8, 8)
                re, im = (local_in[part, b, rows] + own_sign * local[part, b, rows] for part in range(2))
                send[0, b * 16 + t] = jnp.where(lower, re, pltpu.roll(im, 4, 0))
                send[1, b * 16 + t] = jnp.where(lower, pltpu.roll(re, 4, 0), im)

    def spread(src, dst, send_sem, recv_sem, steps=FAR_FIRST):
        for e in steps:

            @pl.loop(0 if e else 1, 8)
            def _(d):
                pz, pw = (z + d) % 8, plane_step(w, e)
                send_to(src.at[pz * 16 + pw], dst.at[me], send_sem, recv_sem, device(pz, pw, core)).start()

    def gathered(src, dst, send_sem, recv_sem):
        return send_to(src.at[pl.ds(0, CHIPS - 1)], dst.at[pl.ds(0, CHIPS - 1)], send_sem, recv_sem, partner)

    def there(k):
        return send.at[k], recv.at[k], there_send.at[k], there_recv.at[k]

    def again(k):
        return back.at[k], back_in.at[k], back_send.at[k], back_recv.at[k]

    pl.semaphore_wait(ready, 15)
    spread(*there(0), steps=FAR_FIRST[:10])
    recv[0, me] = send[0, me]

    for d in (1, 7, 2, 6, 3, 5, 4):
        source = (z + d) % 8
        send_to(
            level.at[0], level_mid.at[source], mid_send, mid_recv.at[7 - d], device(source, w, core)
        ).wait_recv()

    @pl.loop(1, 16)
    def _(e):
        pw = plane_step(w, e)
        send_to(
            level_mid.at[:, pl.ds(pw * 8, 8)], level_in.at[:, w], level_send, level_recv, device(z, pw, core)
        ).start()

    level_in[:, w] = level_mid[:, pl.ds(w * 8, 8)]
    spread(*there(0), steps=FAR_FIRST[10:])
    spread(*there(1))
    recv[1, me] = send[1, me]
    level_part = level_in.at[:, pl.ds(0, 15)]
    level_all = send_to(level_part, level_part, level_send, level_recv, partner)
    level_all.wait_recv()

    @pl.loop(0, 8)
    def _(i):
        c, s = scaled_turn(angle_ref[1:2] * level_in[i].reshape(128, 128))
        cosine[i], sine[i] = c.reshape(16, 8, 128), s.reshape(16, 8, 128)

    sublane = lax.broadcasted_iota(jnp.int32, (8, 128), 0)

    def turn_sublanes(x, step):
        upper = (sublane & step) != 0
        other = jnp.where(upper, pltpu.roll(x, step, 0), pltpu.roll(x, 8 - step, 0))
        return other + jnp.where(upper, -x, x)

    for k in range(2):
        gathered(*there(k)).wait_recv()

        @pl.loop(0, 8)
        def _(i):
            for j, x in enumerate(fwht([recv[k, i * 16 + j] for j in range(16)])):
                recv[k, i * 16 + j] = x

        @pl.loop(0, 16)
        def _(j):
            tiles = fwht([recv[k, i * 16 + j] for i in range(8)])
            for i in range(8):
                c, s = cosine[i, j], sine[i, j]
                if k == 0:
                    c, s = jnp.where(lower, c, pltpu.roll(c, 4, 0)), jnp.where(lower, s, -pltpu.roll(s, 4, 0))
                else:
                    c, s = jnp.where(lower, pltpu.roll(c, 4, 0), c), jnp.where(lower, pltpu.roll(s, 4, 0), -s)
                tiles[i] = tiles[i] * c + pltpu.roll(tiles[i], 4, 0) * s
            for i, x in enumerate(fwht(tiles)):
                recv[k, i * 16 + j] = x

        @pl.loop(0, 8)
        def _(i):
            tiles = fwht([recv[k, i * 16 + j] for j in range(16)])
            tiles = [turn_sublanes(turn_sublanes(x, 1), 2) for x in tiles]
            x = turn_lanes(jnp.concatenate(tiles, axis=0), signs)
            for j in range(16):
                mix[k, i * 16 + j] = x[j * 8 : j * 8 + 8]

        pair = send_to(mix.at[k], mix_in.at[k], pair_send.at[4 + k], pair_recv.at[4 + k], partner)
        pair.start()
        pair.wait()

        @pl.loop(0, 8)
        def _(i):
            for j in range(16):
                t = i * 16 + j
                back[k, t] = mix_in[k, t] + own_sign * mix[k, t]

        spread(*again(k))
        back_in[k, me] = back[k, me]

    for q in range(4):
        swap(q).wait_send()
    for d in range(7):
        send_to(level.at[0], level_mid.at[0], mid_send, mid_recv.at[0], partner).wait_send()
    level_all.wait_send()
    for k in range(2):
        gathered(*there(k)).wait_send()

    for k in range(2):
        gathered(*again(k)).wait_recv()

        @pl.loop(0, 8)
        def _(i):
            for j, x in enumerate(fwht([back_in[k, i * 16 + j] for j in range(16)])):
                out_ref[k, i * 16 + j] = x

    for k in range(2):
        gathered(*again(k)).wait_send()


def finish(tiles_ref, out_ref, final, out_sem):
    lower = lax.broadcasted_iota(jnp.int32, (8, 128), 0) < 4
    copies = []
    for q in range(4):

        @pl.loop(q * 4, q * 4 + 4)
        def _(j):
            first, second = (fwht([tiles_ref[k, i * 16 + j] for i in range(8)]) for k in range(2))
            rows = pl.ds(j * 8, 8)
            for i in range(8):
                u, v = first[i] + second[i], first[i] - second[i]
                final[0, i, rows] = jnp.where(lower, u, pltpu.roll(v, 4, 0))
                final[1, i, rows] = jnp.where(lower, pltpu.roll(u, 4, 0), v)

        rows = pl.ds(q * 32, 32)
        copies.append(pltpu.make_async_copy(final.at[:, :, rows], out_ref.at[:, :, rows], out_sem.at[q]))
        copies[-1].start()
    for copy in copies:
        copy.wait()


def body(wave_parts, level_table, phase_angles):
    f32 = jnp.float32
    state, tiles = pltpu.VMEM((2, 8, 128, 128), f32), pltpu.VMEM((2, CHIPS, 8, 128), f32)
    table = pltpu.VMEM((8, 16, 8, 128), f32)
    blocks = pltpu.VMEM((8, 128, 128), f32)
    dma, regular = pltpu.SemaphoreType.DMA, pltpu.SemaphoreType.REGULAR
    anywhere, on_chip = pl.BlockSpec(memory_space=pl.ANY), pl.BlockSpec(memory_space=pltpu.VMEM)
    off_chip = pl.BlockSpec(memory_space=pltpu.HBM)
    args = [pltpu.with_memory_space_constraint(x, pltpu.HBM) for x in (wave_parts, level_table, phase_angles)]
    mixed = pl.pallas_call(
        kernel,
        out_shape=pltpu.VMEM((2, CHIPS, 8, 128), f32),
        in_specs=[off_chip] * 3,
        out_specs=on_chip,
        scratch_shapes=[
            state, blocks, pltpu.VMEM((2, 128), f32), table, table, state, state, tiles, tiles, blocks, table, tiles, tiles, tiles, tiles,
            dma((3,)), dma((6,)), dma((6,)), dma, dma((7,)), dma, dma, dma((2,)), dma((2,)), dma((2,)), dma((2,)), regular, regular((3,)),
        ],
        compiler_params=pltpu.CompilerParams(collective_id=0, has_side_effects=True, vmem_limit_bytes=32 * 2**20),
    )(*args)
    return pl.pallas_call(
        finish,
        out_shape=jax.ShapeDtypeStruct(wave_parts.shape, f32),
        in_specs=[on_chip],
        out_specs=anywhere,
        scratch_shapes=[state, dma((4,))],
        compiler_params=pltpu.CompilerParams(vmem_limit_bytes=16 * 2**20),
    )(mixed)


def solution(mesh):
    in_specs = (P(None, ("qa", "qb"), None, None), P(("qa", "qb"), None, None), P())
    out_specs = P(None, ("qa", "qb"), None, None)
    return jax.shard_map(body, mesh=mesh, in_specs=in_specs, out_specs=out_specs, check_vma=False)
```

```python
import functools

import jax
import jax.numpy as jnp
from jax import lax
from jax.experimental import pallas as pl
from jax.experimental.pallas import tpu as pltpu
from jax.sharding import PartitionSpec as P

MESH = pl.DeviceIdType.MESH
SCALE = 2.0**-12.5
CHIPS = 128
FAR_FIRST = (5, 3, 7, 12, 13, 1, 4, 10, 11, 14, 15, 2, 6, 8, 9, 0)
COS = (0.9999999995270198, -0.49999999256864547, 0.04166664759094903, -0.0013888705067878636, 2.479313621797957e-05, -2.7357116288633015e-07, 1.850280961043466e-09)
SIN = (0.9999999957579141, -0.1666666176642379, 0.008333241511668515, -0.00019834965410918986, 2.7360914118386437e-06, -2.2205074368871847e-08)


def place():
    qa, qb = lax.axis_index("qa"), lax.axis_index("qb")
    return qa // 4, (qa // 2) % 2 * 8 + qb, qa % 2


def device(z, w, core):
    return (z * 4 + w // 8 * 2 + core, w % 8)


def plane(x, y):
    return x % 2 * 8 + y * 2 + x // 2


def plane_step(w, d):
    xlo = (w // 8 + d // 8) % 2
    y = (w // 2 % 4 + d // 2 % 4) % 4
    xhi = (w % 2 + d % 2) % 2
    return xlo * 8 + y * 2 + xhi


def fwht(tiles):
    tiles = list(tiles)
    step = 1
    while step < len(tiles):
        for i in range(len(tiles)):
            if not i & step:
                u, v = tiles[i], tiles[i + step]
                tiles[i], tiles[i + step] = u + v, u - v
        step *= 2
    return tiles


def polynomial(terms, x):
    value = terms[-1] * SCALE
    for term in terms[-2::-1]:
        value = value * x + term * SCALE
    return value


def scaled_turn(turn):
    square = turn * turn
    return polynomial(COS, square), turn * polynomial(SIN, square)


def sign_matrix(count):
    both = lax.broadcasted_iota(jnp.int32, (count, count), 0) & lax.broadcasted_iota(jnp.int32, (count, count), 1)
    for shift in (4, 2, 1):
        both = both ^ (both >> shift)
    return (1 - 2 * (both & 1)).astype(jnp.float32).astype(jnp.bfloat16)


def halves(x):
    high = x.astype(jnp.bfloat16)
    return high, (x - high.astype(jnp.float32)).astype(jnp.bfloat16)


def turn_lanes(x, signs):
    high, low = halves(x)
    dot = functools.partial(jnp.dot, preferred_element_type=jnp.float32)
    return dot(high, signs) + dot(low, signs)


def turn_rows(x, signs):
    high, low = halves(x)
    dot = functools.partial(jnp.dot, preferred_element_type=jnp.float32)
    return dot(signs, high) + dot(signs, low)


def kernel(
    wave_ref, level_ref, angle_hbm, out_ref,
    wave, level, angle_ref, cosine, sine, local, local_in, send, recv, level_mid, level_in, mix, mix_in, back, back_in,
    in_sem, pair_send, pair_recv, mid_send, mid_recv, level_send, level_recv, there_send, there_recv, back_send, back_recv, ready, beside, far,
):
    z, w, core = place()
    me = z * 16 + w
    partner = device(z, w, 1 - core)
    own_sign = (1 - 2 * core).astype(jnp.float32)
    lower = lax.broadcasted_iota(jnp.int32, (8, 128), 0) < 4

    barrier = pltpu.get_barrier_semaphore()

    def signal(sem, to):
        pl.semaphore_signal(sem, inc=1, device_id=to, device_id_type=MESH)

    def send_to(src, dst, send_sem, recv_sem, to):
        return pltpu.make_async_remote_copy(src, dst, send_sem, recv_sem, device_id=to, device_id_type=MESH)

    level_copy = pltpu.make_async_copy(level_ref, level, in_sem.at[0])
    wave_copy = pltpu.make_async_copy(wave_ref, wave, in_sem.at[1])
    level_copy.start()
    angle_copy = pltpu.make_async_copy(angle_hbm, angle_ref, in_sem.at[2])
    angle_copy.start()
    wave_copy.start()

    x, y = w % 2 * 2 + w // 8, w // 2 % 4
    y_both = [device(z, plane(x, (y + d) % 4), core) for d in (1, 3)]
    x_both = [device(z, plane((x + d) % 4, y), core) for d in (1, 3)]
    for to in [device((z + d) % 8, w, core) for d in (2, 6, 1, 7)] + y_both + x_both + [partner]:
        signal(barrier, to)

    signs = sign_matrix(128)

    def send_levels(d):
        there = (z + d) % 8
        send_to(level.at[there], level_mid.at[z], mid_send, mid_recv.at[d - 1], device(there, w, core)).start()

    def first_turns(start, stop):
        @pl.loop(start, stop)
        def _(b):
            c, s = scaled_turn(angle_ref[0:1] * level[b])
            re, im = wave[0, b], wave[1, b]
            for part, value in enumerate((re * c + im * s, im * c - re * s)):
                local[part, b] = turn_rows(turn_lanes(value, signs), signs)

    pl.semaphore_wait(barrier, 9)
    for i, d in enumerate((7, 1, 6)):
        signal(far.at[i], device((z + d) % 8, w, core))
    level_copy.wait()
    for d in (1, 7, 2, 6):
        send_levels(d)
    for to in y_both:
        signal(beside.at[0], to)
    angle_copy.wait()
    wave_copy.wait()
    first_turns(0, 2)
    for i, d in enumerate((3, 5, 4)):
        pl.semaphore_wait(far.at[i], 1)
        send_levels(d)
    for step in range(2):
        pl.semaphore_wait(beside.at[step], 2)
        for to in x_both:
            signal(beside.at[step + 1], to)
        first_turns(2 + step * 2, 4 + step * 2)
    pl.semaphore_wait(beside.at[2], 2)

    @pl.loop(1, 16)
    def _(d):
        signal(ready, device(z, plane_step(w, d), core))

    first_turns(6, 8)
    level_mid[z] = level[z]

    def swap(q):
        rows = pl.ds(q * 32, 32)
        return send_to(
            local.at[:, :, rows], local_in.at[:, :, rows], pair_send.at[q], pair_recv.at[q], partner
        )

    for q in range(4):

        @pl.loop(q * 4, q * 4 + 4)
        def _(t):
            rows = pl.ds(t * 8, 8)
            for part in range(2):
                for b, x in enumerate(fwht([local[part, b, rows] for b in range(8)])):
                    local[part, b, rows] = x

        swap(q).start()

    for q in range(4):
        swap(q).wait_recv()

        @pl.loop(0, 8)
        def _(b):
            for t in range(q * 4, q * 4 + 4):
                rows = pl.ds(t * 8, 8)
                re, im = (local_in[part, b, rows] + own_sign * local[part, b, rows] for part in range(2))
                send[0, b * 16 + t] = jnp.where(lower, re, pltpu.roll(im, 4, 0))
                send[1, b * 16 + t] = jnp.where(lower, pltpu.roll(re, 4, 0), im)

    def spread(src, dst, send_sem, recv_sem, steps=FAR_FIRST):
        for e in steps:

            @pl.loop(0 if e else 1, 8)
            def _(d):
                pz, pw = (z + d) % 8, plane_step(w, e)
                send_to(src.at[pz * 16 + pw], dst.at[me], send_sem, recv_sem, device(pz, pw, core)).start()

    def gathered(src, dst, send_sem, recv_sem):
        return send_to(src.at[pl.ds(0, CHIPS - 1)], dst.at[pl.ds(0, CHIPS - 1)], send_sem, recv_sem, partner)

    def there(k):
        return send.at[k], recv.at[k], there_send.at[k], there_recv.at[k]

    def again(k):
        return back.at[k], back_in.at[k], back_send.at[k], back_recv.at[k]

    pl.semaphore_wait(ready, 15)
    spread(*there(0), steps=FAR_FIRST[:13])
    recv[0, me] = send[0, me]

    for d in (1, 7, 2, 6, 3, 5, 4):
        source = (z + d) % 8
        send_to(
            level.at[0], level_mid.at[source], mid_send, mid_recv.at[7 - d], device(source, w, core)
        ).wait_recv()

    @pl.loop(1, 16)
    def _(e):
        pw = plane_step(w, e)
        send_to(
            level_mid.at[:, pl.ds(pw * 8, 8)], level_in.at[:, w], level_send, level_recv, device(z, pw, core)
        ).start()

    level_in[:, w] = level_mid[:, pl.ds(w * 8, 8)]
    spread(*there(0), steps=FAR_FIRST[13:])
    spread(*there(1))
    recv[1, me] = send[1, me]
    level_part = level_in.at[:, pl.ds(0, 15)]
    level_all = send_to(level_part, level_part, level_send, level_recv, partner)
    level_all.wait_recv()

    @pl.loop(0, 8)
    def _(i):
        c, s = scaled_turn(angle_ref[1:2] * level_in[i].reshape(128, 128))
        cosine[i], sine[i] = c.reshape(16, 8, 128), s.reshape(16, 8, 128)

    sublane = lax.broadcasted_iota(jnp.int32, (8, 128), 0)

    def turn_sublanes(x, step):
        upper = (sublane & step) != 0
        other = jnp.where(upper, pltpu.roll(x, step, 0), pltpu.roll(x, 8 - step, 0))
        return other + jnp.where(upper, -x, x)

    for k in range(2):
        gathered(*there(k)).wait_recv()

        @pl.loop(0, 8)
        def _(i):
            for j, x in enumerate(fwht([recv[k, i * 16 + j] for j in range(16)])):
                recv[k, i * 16 + j] = x

        @pl.loop(0, 16)
        def _(j):
            tiles = fwht([recv[k, i * 16 + j] for i in range(8)])
            for i in range(8):
                c, s = cosine[i, j], sine[i, j]
                if k == 0:
                    c, s = jnp.where(lower, c, pltpu.roll(c, 4, 0)), jnp.where(lower, s, -pltpu.roll(s, 4, 0))
                else:
                    c, s = jnp.where(lower, pltpu.roll(c, 4, 0), c), jnp.where(lower, pltpu.roll(s, 4, 0), -s)
                tiles[i] = tiles[i] * c + pltpu.roll(tiles[i], 4, 0) * s
            for i, x in enumerate(fwht(tiles)):
                recv[k, i * 16 + j] = x

        @pl.loop(0, 8)
        def _(i):
            tiles = fwht([recv[k, i * 16 + j] for j in range(16)])
            tiles = [turn_sublanes(turn_sublanes(x, 1), 2) for x in tiles]
            x = turn_lanes(jnp.concatenate(tiles, axis=0), signs)
            for j in range(16):
                mix[k, i * 16 + j] = x[j * 8 : j * 8 + 8]

        pair = send_to(mix.at[k], mix_in.at[k], pair_send.at[4 + k], pair_recv.at[4 + k], partner)
        pair.start()
        pair.wait()

        @pl.loop(0, 8)
        def _(i):
            for j in range(16):
                t = i * 16 + j
                back[k, t] = mix_in[k, t] + own_sign * mix[k, t]

        spread(*again(k))
        back_in[k, me] = back[k, me]

    for q in range(4):
        swap(q).wait_send()
    for d in range(7):
        send_to(level.at[0], level_mid.at[0], mid_send, mid_recv.at[0], partner).wait_send()
    level_all.wait_send()
    for k in range(2):
        gathered(*there(k)).wait_send()

    for k in range(2):
        gathered(*again(k)).wait_recv()

        @pl.loop(0, 8)
        def _(i):
            for j, x in enumerate(fwht([back_in[k, i * 16 + j] for j in range(16)])):
                out_ref[k, i * 16 + j] = x

        if k == 0:

            @pl.loop(0, 16)
            def _(j):
                for i, x in enumerate(fwht([out_ref[k, i * 16 + j] for i in range(8)])):
                    out_ref[k, i * 16 + j] = x

    for k in range(2):
        gathered(*again(k)).wait_send()


def finish(tiles_ref, out_ref, final, out_sem):
    lower = lax.broadcasted_iota(jnp.int32, (8, 128), 0) < 4
    copies = []
    for q in range(8):

        @pl.loop(q * 2, q * 2 + 2)
        def _(j):
            first, second = ([tiles_ref[k, i * 16 + j] for i in range(8)] for k in range(2))
            second = fwht(second)
            rows = pl.ds(j * 8, 8)
            for i in range(8):
                u, v = first[i] + second[i], first[i] - second[i]
                final[0, i, rows] = jnp.where(lower, u, pltpu.roll(v, 4, 0))
                final[1, i, rows] = jnp.where(lower, pltpu.roll(u, 4, 0), v)

        rows = pl.ds(q * 16, 16)
        copies.append(pltpu.make_async_copy(final.at[:, :, rows], out_ref.at[:, :, rows], out_sem.at[q]))
        copies[-1].start()
    for copy in copies:
        copy.wait()


def body(wave_parts, level_table, phase_angles):
    f32 = jnp.float32
    state, tiles = pltpu.VMEM((2, 8, 128, 128), f32), pltpu.VMEM((2, CHIPS, 8, 128), f32)
    table = pltpu.VMEM((8, 16, 8, 128), f32)
    blocks = pltpu.VMEM((8, 128, 128), f32)
    dma, regular = pltpu.SemaphoreType.DMA, pltpu.SemaphoreType.REGULAR
    anywhere, on_chip = pl.BlockSpec(memory_space=pl.ANY), pl.BlockSpec(memory_space=pltpu.VMEM)
    off_chip = pl.BlockSpec(memory_space=pltpu.HBM)
    args = [pltpu.with_memory_space_constraint(x, pltpu.HBM) for x in (wave_parts, level_table, phase_angles)]
    mixed = pl.pallas_call(
        kernel,
        out_shape=pltpu.VMEM((2, CHIPS, 8, 128), f32),
        in_specs=[off_chip] * 3,
        out_specs=on_chip,
        scratch_shapes=[
            state, blocks, pltpu.VMEM((2, 128), f32), table, table, state, state, tiles, tiles, blocks, table, tiles, tiles, tiles, tiles,
            dma((3,)), dma((6,)), dma((6,)), dma, dma((7,)), dma, dma, dma((2,)), dma((2,)), dma((2,)), dma((2,)), regular, regular((3,)), regular((3,)),
        ],
        compiler_params=pltpu.CompilerParams(collective_id=0, has_side_effects=True, vmem_limit_bytes=32 * 2**20),
    )(*args)
    return pl.pallas_call(
        finish,
        out_shape=jax.ShapeDtypeStruct(wave_parts.shape, f32),
        in_specs=[on_chip],
        out_specs=anywhere,
        scratch_shapes=[state, dma((8,))],
        compiler_params=pltpu.CompilerParams(vmem_limit_bytes=16 * 2**20),
    )(mixed)


def solution(mesh):
    in_specs = (P(None, ("qa", "qb"), None, None), P(("qa", "qb"), None, None), P())
    out_specs = P(None, ("qa", "qb"), None, None)
    return jax.shard_map(body, mesh=mesh, in_specs=in_specs, out_specs=out_specs, check_vma=False)
```

```python
import functools

import jax
import jax.numpy as jnp
from jax import lax
from jax.experimental import pallas as pl
from jax.experimental.pallas import tpu as pltpu
from jax.sharding import PartitionSpec as P

MESH = pl.DeviceIdType.MESH
SCALE = 2.0**-12.5
CHIPS = 128
FAR_FIRST = (5, 3, 7, 12, 13, 1, 4, 10, 11, 14, 15, 2, 6, 8, 9, 0)
COS = (0.9999999995270198, -0.49999999256864547, 0.04166664759094903, -0.0013888705067878636, 2.479313621797957e-05, -2.7357116288633015e-07, 1.850280961043466e-09)
SIN = (0.9999999957579141, -0.1666666176642379, 0.008333241511668515, -0.00019834965410918986, 2.7360914118386437e-06, -2.2205074368871847e-08)


def place():
    qa, qb = lax.axis_index("qa"), lax.axis_index("qb")
    return qa // 4, (qa // 2) % 2 * 8 + qb, qa % 2


def device(z, w, core):
    return (z * 4 + w // 8 * 2 + core, w % 8)


def plane(x, y):
    return x % 2 * 8 + y * 2 + x // 2


def plane_step(w, d):
    xlo = (w // 8 + d // 8) % 2
    y = (w // 2 % 4 + d // 2 % 4) % 4
    xhi = (w % 2 + d % 2) % 2
    return xlo * 8 + y * 2 + xhi


def fwht(tiles):
    tiles = list(tiles)
    step = 1
    while step < len(tiles):
        for i in range(len(tiles)):
            if not i & step:
                u, v = tiles[i], tiles[i + step]
                tiles[i], tiles[i + step] = u + v, u - v
        step *= 2
    return tiles


def polynomial(terms, x):
    value = terms[-1] * SCALE
    for term in terms[-2::-1]:
        value = value * x + term * SCALE
    return value


def scaled_turn(turn):
    square = turn * turn
    return polynomial(COS, square), turn * polynomial(SIN, square)


def sign_matrix(count):
    both = lax.broadcasted_iota(jnp.int32, (count, count), 0) & lax.broadcasted_iota(jnp.int32, (count, count), 1)
    for shift in (4, 2, 1):
        both = both ^ (both >> shift)
    return (1 - 2 * (both & 1)).astype(jnp.float32).astype(jnp.bfloat16)


def halves(x):
    high = x.astype(jnp.bfloat16)
    return high, (x - high.astype(jnp.float32)).astype(jnp.bfloat16)


def turn_lanes(x, signs):
    high, low = halves(x)
    dot = functools.partial(jnp.dot, preferred_element_type=jnp.float32)
    return dot(high, signs) + dot(low, signs)


def turn_rows(x, signs):
    high, low = halves(x)
    dot = functools.partial(jnp.dot, preferred_element_type=jnp.float32)
    return dot(signs, high) + dot(signs, low)


def kernel(
    wave_ref, level_ref, angle_hbm, out_ref,
    wave, level, angle_ref, cosine, sine, local, local_in, send, recv, level_mid, level_in, mix, mix_in, back, back_in,
    in_sem, pair_send, pair_recv, mid_send, mid_recv, level_send, level_recv, there_send, there_recv, back_send, back_recv, ready, beside, far,
):
    z, w, core = place()
    me = z * 16 + w
    partner = device(z, w, 1 - core)
    own_sign = (1 - 2 * core).astype(jnp.float32)
    lower = lax.broadcasted_iota(jnp.int32, (8, 128), 0) < 4

    barrier = pltpu.get_barrier_semaphore()

    def signal(sem, to):
        pl.semaphore_signal(sem, inc=1, device_id=to, device_id_type=MESH)

    def send_to(src, dst, send_sem, recv_sem, to):
        return pltpu.make_async_remote_copy(src, dst, send_sem, recv_sem, device_id=to, device_id_type=MESH)

    level_copy = pltpu.make_async_copy(level_ref, level, in_sem.at[0])
    wave_copy = pltpu.make_async_copy(wave_ref, wave, in_sem.at[1])
    level_copy.start()
    angle_copy = pltpu.make_async_copy(angle_hbm, angle_ref, in_sem.at[2])
    angle_copy.start()

    x, y = w % 2 * 2 + w // 8, w // 2 % 4
    y_both = [device(z, plane(x, (y + d) % 4), core) for d in (1, 3)]
    x_both = [device(z, plane((x + d) % 4, y), core) for d in (1, 3)]
    for to in [device((z + d) % 8, w, core) for d in (2, 6, 1, 7)] + y_both + x_both + [partner]:
        signal(barrier, to)

    wave_copy.start()
    signs = sign_matrix(128)

    def send_levels(d):
        there = (z + d) % 8
        send_to(level.at[there], level_mid.at[z], mid_send, mid_recv.at[d - 1], device(there, w, core)).start()

    def first_turns(start, stop):
        @pl.loop(start, stop)
        def _(b):
            c, s = scaled_turn(angle_ref[0:1] * level[b])
            re, im = wave[0, b], wave[1, b]
            for part, value in enumerate((re * c + im * s, im * c - re * s)):
                local[part, b] = turn_rows(turn_lanes(value, signs), signs)

    pl.semaphore_wait(barrier, 9)
    for i, d in enumerate((7, 1, 6)):
        signal(far.at[i], device((z + d) % 8, w, core))
    level_copy.wait()
    for d in (1, 7, 2, 6):
        send_levels(d)
    for to in y_both:
        signal(beside.at[0], to)
    angle_copy.wait()
    wave_copy.wait()
    first_turns(0, 2)
    for i, d in enumerate((3, 5, 4)):
        pl.semaphore_wait(far.at[i], 1)
        send_levels(d)
    for step in range(2):
        pl.semaphore_wait(beside.at[step], 2)
        for to in x_both:
            signal(beside.at[step + 1], to)
        first_turns(2 + step * 2, 4 + step * 2)
    pl.semaphore_wait(beside.at[2], 2)

    @pl.loop(1, 16)
    def _(d):
        signal(ready, device(z, plane_step(w, d), core))

    first_turns(6, 8)
    level_mid[z] = level[z]

    def swap(q):
        rows = pl.ds(q * 32, 32)
        return send_to(
            local.at[:, :, rows], local_in.at[:, :, rows], pair_send.at[q], pair_recv.at[q], partner
        )

    for q in range(4):

        @pl.loop(q * 4, q * 4 + 4)
        def _(t):
            rows = pl.ds(t * 8, 8)
            for part in range(2):
                for b, x in enumerate(fwht([local[part, b, rows] for b in range(8)])):
                    local[part, b, rows] = x

        swap(q).start()

    for q in range(4):
        swap(q).wait_recv()

        @pl.loop(0, 8)
        def _(b):
            for t in range(q * 4, q * 4 + 4):
                rows = pl.ds(t * 8, 8)
                re, im = (local_in[part, b, rows] + own_sign * local[part, b, rows] for part in range(2))
                send[0, b * 16 + t] = jnp.where(lower, re, pltpu.roll(im, 4, 0))
                send[1, b * 16 + t] = jnp.where(lower, pltpu.roll(re, 4, 0), im)

    def spread(src, dst, send_sem, recv_sem, steps=FAR_FIRST):
        for e in steps:

            @pl.loop(0 if e else 1, 8)
            def _(d):
                pz, pw = (z + d) % 8, plane_step(w, e)
                send_to(src.at[pz * 16 + pw], dst.at[me], send_sem, recv_sem, device(pz, pw, core)).start()

    def gathered(src, dst, send_sem, recv_sem):
        return send_to(src.at[pl.ds(0, CHIPS - 1)], dst.at[pl.ds(0, CHIPS - 1)], send_sem, recv_sem, partner)

    def there(k):
        return send.at[k], recv.at[k], there_send.at[k], there_recv.at[k]

    def again(k):
        return back.at[k], back_in.at[k], back_send.at[k], back_recv.at[k]

    pl.semaphore_wait(ready, 15)
    spread(*there(0), steps=FAR_FIRST[:13])
    recv[0, me] = send[0, me]

    for d in (1, 7, 2, 6, 3, 5, 4):
        source = (z + d) % 8
        send_to(
            level.at[0], level_mid.at[source], mid_send, mid_recv.at[7 - d], device(source, w, core)
        ).wait_recv()

    @pl.loop(1, 16)
    def _(e):
        pw = plane_step(w, e)
        send_to(
            level_mid.at[:, pl.ds(pw * 8, 8)], level_in.at[:, w], level_send, level_recv, device(z, pw, core)
        ).start()

    level_in[:, w] = level_mid[:, pl.ds(w * 8, 8)]
    spread(*there(0), steps=FAR_FIRST[13:])
    spread(*there(1))
    recv[1, me] = send[1, me]
    level_part = level_in.at[:, pl.ds(0, 15)]
    level_all = send_to(level_part, level_part, level_send, level_recv, partner)
    level_all.wait_recv()

    @pl.loop(0, 8)
    def _(i):
        c, s = scaled_turn(angle_ref[1:2] * level_in[i].reshape(128, 128))
        cosine[i], sine[i] = c.reshape(16, 8, 128), s.reshape(16, 8, 128)

    sublane = lax.broadcasted_iota(jnp.int32, (8, 128), 0)

    def turn_sublanes(x, step):
        upper = (sublane & step) != 0
        other = jnp.where(upper, pltpu.roll(x, step, 0), pltpu.roll(x, 8 - step, 0))
        return other + jnp.where(upper, -x, x)

    for k in range(2):
        gathered(*there(k)).wait_recv()

        @pl.loop(0, 8)
        def _(i):
            for j, x in enumerate(fwht([recv[k, i * 16 + j] for j in range(16)])):
                recv[k, i * 16 + j] = x

        @pl.loop(0, 16)
        def _(j):
            tiles = fwht([recv[k, i * 16 + j] for i in range(8)])
            for i in range(8):
                c, s = cosine[i, j], sine[i, j]
                if k == 0:
                    c, s = jnp.where(lower, c, pltpu.roll(c, 4, 0)), jnp.where(lower, s, -pltpu.roll(s, 4, 0))
                else:
                    c, s = jnp.where(lower, pltpu.roll(c, 4, 0), c), jnp.where(lower, pltpu.roll(s, 4, 0), -s)
                tiles[i] = tiles[i] * c + pltpu.roll(tiles[i], 4, 0) * s
            for i, x in enumerate(fwht(tiles)):
                recv[k, i * 16 + j] = x

        @pl.loop(0, 8)
        def _(i):
            tiles = fwht([recv[k, i * 16 + j] for j in range(16)])
            tiles = [turn_sublanes(turn_sublanes(x, 1), 2) for x in tiles]
            x = turn_lanes(jnp.concatenate(tiles, axis=0), signs)
            for j in range(16):
                mix[k, i * 16 + j] = x[j * 8 : j * 8 + 8]

        pair = send_to(mix.at[k], mix_in.at[k], pair_send.at[4 + k], pair_recv.at[4 + k], partner)
        pair.start()
        pair.wait()

        @pl.loop(0, 8)
        def _(i):
            for j in range(16):
                t = i * 16 + j
                back[k, t] = mix_in[k, t] + own_sign * mix[k, t]

        spread(*again(k))
        back_in[k, me] = back[k, me]

    for q in range(4):
        swap(q).wait_send()
    for d in range(7):
        send_to(level.at[0], level_mid.at[0], mid_send, mid_recv.at[0], partner).wait_send()
    level_all.wait_send()
    for k in range(2):
        gathered(*there(k)).wait_send()

    for k in range(2):
        gathered(*again(k)).wait_recv()

        @pl.loop(0, 8)
        def _(i):
            for j, x in enumerate(fwht([back_in[k, i * 16 + j] for j in range(16)])):
                out_ref[k, i * 16 + j] = x

        if k == 0:

            @pl.loop(0, 16)
            def _(j):
                for i, x in enumerate(fwht([out_ref[k, i * 16 + j] for i in range(8)])):
                    out_ref[k, i * 16 + j] = x

    for k in range(2):
        gathered(*again(k)).wait_send()


def finish(tiles_ref, out_ref, final, out_sem):
    lower = lax.broadcasted_iota(jnp.int32, (8, 128), 0) < 4
    copies = []
    for q in range(8):

        @pl.loop(q * 2, q * 2 + 2)
        def _(j):
            first, second = ([tiles_ref[k, i * 16 + j] for i in range(8)] for k in range(2))
            second = fwht(second)
            rows = pl.ds(j * 8, 8)
            for i in range(8):
                u, v = first[i] + second[i], first[i] - second[i]
                final[0, i, rows] = jnp.where(lower, u, pltpu.roll(v, 4, 0))
                final[1, i, rows] = jnp.where(lower, pltpu.roll(u, 4, 0), v)

        rows = pl.ds(q * 16, 16)
        copies.append(pltpu.make_async_copy(final.at[:, :, rows], out_ref.at[:, :, rows], out_sem.at[q]))
        copies[-1].start()
    for copy in copies:
        copy.wait()


def body(wave_parts, level_table, phase_angles):
    f32 = jnp.float32
    state, tiles = pltpu.VMEM((2, 8, 128, 128), f32), pltpu.VMEM((2, CHIPS, 8, 128), f32)
    table = pltpu.VMEM((8, 16, 8, 128), f32)
    blocks = pltpu.VMEM((8, 128, 128), f32)
    dma, regular = pltpu.SemaphoreType.DMA, pltpu.SemaphoreType.REGULAR
    anywhere, on_chip = pl.BlockSpec(memory_space=pl.ANY), pl.BlockSpec(memory_space=pltpu.VMEM)
    off_chip = pl.BlockSpec(memory_space=pltpu.HBM)
    args = [pltpu.with_memory_space_constraint(x, pltpu.HBM) for x in (wave_parts, level_table, phase_angles)]
    mixed = pl.pallas_call(
        kernel,
        out_shape=pltpu.VMEM((2, CHIPS, 8, 128), f32),
        in_specs=[off_chip] * 3,
        out_specs=on_chip,
        scratch_shapes=[
            state, blocks, pltpu.VMEM((2, 128), f32), table, table, state, state, tiles, tiles, blocks, table, tiles, tiles, tiles, tiles,
            dma((3,)), dma((6,)), dma((6,)), dma, dma((7,)), dma, dma, dma((2,)), dma((2,)), dma((2,)), dma((2,)), regular, regular((3,)), regular((3,)),
        ],
        compiler_params=pltpu.CompilerParams(collective_id=0, has_side_effects=True, vmem_limit_bytes=32 * 2**20),
    )(*args)
    return pl.pallas_call(
        finish,
        out_shape=jax.ShapeDtypeStruct(wave_parts.shape, f32),
        in_specs=[on_chip],
        out_specs=anywhere,
        scratch_shapes=[state, dma((8,))],
        compiler_params=pltpu.CompilerParams(vmem_limit_bytes=16 * 2**20),
    )(mixed)


def solution(mesh):
    in_specs = (P(None, ("qa", "qb"), None, None), P(("qa", "qb"), None, None), P())
    out_specs = P(None, ("qa", "qb"), None, None)
    return jax.shard_map(body, mesh=mesh, in_specs=in_specs, out_specs=out_specs, check_vma=False)
```

```python
import functools

import jax
import jax.numpy as jnp
from jax import lax
from jax.experimental import pallas as pl
from jax.experimental.pallas import tpu as pltpu
from jax.sharding import PartitionSpec as P

MESH = pl.DeviceIdType.MESH
SCALE = 2.0**-12.5
CHIPS = 128
FAR_FIRST = (5, 3, 7, 12, 13, 1, 4, 10, 11, 14, 15, 2, 6, 8, 9, 0)
COS = (0.9999999995270198, -0.49999999256864547, 0.04166664759094903, -0.0013888705067878636, 2.479313621797957e-05, -2.7357116288633015e-07, 1.850280961043466e-09)
SIN = (0.9999999957579141, -0.1666666176642379, 0.008333241511668515, -0.00019834965410918986, 2.7360914118386437e-06, -2.2205074368871847e-08)


def place():
    qa, qb = lax.axis_index("qa"), lax.axis_index("qb")
    return qa // 4, (qa // 2) % 2 * 8 + qb, qa % 2


def device(z, w, core):
    return (z * 4 + w // 8 * 2 + core, w % 8)


def plane(x, y):
    return x % 2 * 8 + y * 2 + x // 2


def plane_step(w, d):
    xlo = (w // 8 + d // 8) % 2
    y = (w // 2 % 4 + d // 2 % 4) % 4
    xhi = (w % 2 + d % 2) % 2
    return xlo * 8 + y * 2 + xhi


def fwht(tiles):
    tiles = list(tiles)
    step = 1
    while step < len(tiles):
        for i in range(len(tiles)):
            if not i & step:
                u, v = tiles[i], tiles[i + step]
                tiles[i], tiles[i + step] = u + v, u - v
        step *= 2
    return tiles


def polynomial(terms, x):
    value = terms[-1] * SCALE
    for term in terms[-2::-1]:
        value = value * x + term * SCALE
    return value


def scaled_turn(turn):
    square = turn * turn
    return polynomial(COS, square), turn * polynomial(SIN, square)


def sign_matrix(count):
    both = lax.broadcasted_iota(jnp.int32, (count, count), 0) & lax.broadcasted_iota(jnp.int32, (count, count), 1)
    for shift in (4, 2, 1):
        both = both ^ (both >> shift)
    return (1 - 2 * (both & 1)).astype(jnp.float32).astype(jnp.bfloat16)


def halves(x):
    high = x.astype(jnp.bfloat16)
    return high, (x - high.astype(jnp.float32)).astype(jnp.bfloat16)


def turn_lanes(x, signs):
    high, low = halves(x)
    dot = functools.partial(jnp.dot, preferred_element_type=jnp.float32)
    return dot(high, signs) + dot(low, signs)


def turn_rows(x, signs):
    high, low = halves(x)
    dot = functools.partial(jnp.dot, preferred_element_type=jnp.float32)
    return dot(signs, high) + dot(signs, low)


def kernel(
    wave_ref, level_ref, angle_hbm, out_ref,
    wave, level, angle_ref, cosine, sine, local, local_in, send, recv, level_mid, level_in, mix, mix_in, back, back_in,
    in_sem, pair_send, pair_recv, mid_send, mid_recv, level_send, level_recv, there_send, there_recv, back_send, back_recv, ready, beside, far,
):
    z, w, core = place()
    me = z * 16 + w
    partner = device(z, w, 1 - core)
    own_sign = (1 - 2 * core).astype(jnp.float32)
    lower = lax.broadcasted_iota(jnp.int32, (8, 128), 0) < 4

    barrier = pltpu.get_barrier_semaphore()

    def signal(sem, to):
        pl.semaphore_signal(sem, inc=1, device_id=to, device_id_type=MESH)

    def send_to(src, dst, send_sem, recv_sem, to):
        return pltpu.make_async_remote_copy(src, dst, send_sem, recv_sem, device_id=to, device_id_type=MESH)

    level_copy = pltpu.make_async_copy(level_ref, level, in_sem.at[0])
    wave_copy = pltpu.make_async_copy(wave_ref, wave, in_sem.at[1])
    level_copy.start()
    angle_copy = pltpu.make_async_copy(angle_hbm, angle_ref, in_sem.at[2])
    angle_copy.start()

    x, y = w % 2 * 2 + w // 8, w // 2 % 4
    y_both = [device(z, plane(x, (y + d) % 4), core) for d in (1, 3)]
    x_both = [device(z, plane((x + d) % 4, y), core) for d in (1, 3)]
    for to in [device((z + d) % 8, w, core) for d in (2, 6, 1, 7)] + y_both + x_both + [partner]:
        signal(barrier, to)

    wave_copy.start()
    signs = sign_matrix(128)

    def send_levels(d):
        there = (z + d) % 8
        send_to(level.at[there], level_mid.at[z], mid_send, mid_recv.at[d - 1], device(there, w, core)).start()

    def first_turns(start, stop):
        @pl.loop(start, stop)
        def _(b):
            c, s = scaled_turn(angle_ref[0:1] * level[b])
            re, im = wave[0, b], wave[1, b]
            for part, value in enumerate((re * c + im * s, im * c - re * s)):
                local[part, b] = turn_rows(turn_lanes(value, signs), signs)

    pl.semaphore_wait(barrier, 9)
    for i, d in enumerate((7, 1, 6)):
        signal(far.at[i], device((z + d) % 8, w, core))
    level_copy.wait()
    for d in (1, 7, 2, 6):
        send_levels(d)
    for to in y_both:
        signal(beside.at[0], to)
    angle_copy.wait()
    wave_copy.wait()
    first_turns(0, 2)
    for i, d in enumerate((3, 5, 4)):
        pl.semaphore_wait(far.at[i], 1)
        send_levels(d)
    for step in range(2):
        pl.semaphore_wait(beside.at[step], 2)
        for to in x_both:
            signal(beside.at[step + 1], to)
        first_turns(2 + step * 2, 4 + step * 2)
    pl.semaphore_wait(beside.at[2], 2)

    @pl.loop(1, 16)
    def _(d):
        signal(ready, device(z, plane_step(w, d), core))

    first_turns(6, 8)
    level_mid[z] = level[z]

    def swap(q):
        rows = pl.ds(q * 32, 32)
        return send_to(
            local.at[:, :, rows], local_in.at[:, :, rows], pair_send.at[q], pair_recv.at[q], partner
        )

    for q in range(4):

        @pl.loop(q * 4, q * 4 + 4)
        def _(t):
            rows = pl.ds(t * 8, 8)
            for part in range(2):
                for b, x in enumerate(fwht([local[part, b, rows] for b in range(8)])):
                    local[part, b, rows] = x

        swap(q).start()

    for q in range(4):
        swap(q).wait_recv()

        @pl.loop(0, 8)
        def _(b):
            for t in range(q * 4, q * 4 + 4):
                rows = pl.ds(t * 8, 8)
                re, im = (local_in[part, b, rows] + own_sign * local[part, b, rows] for part in range(2))
                send[0, b * 16 + t] = jnp.where(lower, re, pltpu.roll(im, 4, 0))
                send[1, b * 16 + t] = jnp.where(lower, pltpu.roll(re, 4, 0), im)

    def spread(src, dst, send_sem, recv_sem, steps=FAR_FIRST):
        for e in steps:

            @pl.loop(0 if e else 1, 8)
            def _(d):
                pz, pw = (z + d + (core * 4 if e else 0)) % 8, plane_step(w, e)
                send_to(src.at[pz * 16 + pw], dst.at[me], send_sem, recv_sem, device(pz, pw, core)).start()

    def gathered(src, dst, send_sem, recv_sem):
        return send_to(src.at[pl.ds(0, CHIPS - 1)], dst.at[pl.ds(0, CHIPS - 1)], send_sem, recv_sem, partner)

    def there(k):
        return send.at[k], recv.at[k], there_send.at[k], there_recv.at[k]

    def again(k):
        return back.at[k], back_in.at[k], back_send.at[k], back_recv.at[k]

    pl.semaphore_wait(ready, 15)
    spread(*there(0), steps=FAR_FIRST[:13])
    recv[0, me] = send[0, me]

    for d in (1, 7, 2, 6, 3, 5, 4):
        source = (z + d) % 8
        send_to(
            level.at[0], level_mid.at[source], mid_send, mid_recv.at[7 - d], device(source, w, core)
        ).wait_recv()

    @pl.loop(1, 16)
    def _(e):
        pw = plane_step(w, e)
        send_to(
            level_mid.at[:, pl.ds(pw * 8, 8)], level_in.at[:, w], level_send, level_recv, device(z, pw, core)
        ).start()

    level_in[:, w] = level_mid[:, pl.ds(w * 8, 8)]
    spread(*there(0), steps=FAR_FIRST[13:])
    spread(*there(1))
    recv[1, me] = send[1, me]
    level_part = level_in.at[:, pl.ds(0, 15)]
    level_all = send_to(level_part, level_part, level_send, level_recv, partner)
    level_all.wait_recv()

    @pl.loop(0, 8)
    def _(i):
        c, s = scaled_turn(angle_ref[1:2] * level_in[i].reshape(128, 128))
        cosine[i], sine[i] = c.reshape(16, 8, 128), s.reshape(16, 8, 128)

    sublane = lax.broadcasted_iota(jnp.int32, (8, 128), 0)

    def turn_sublanes(x, step):
        upper = (sublane & step) != 0
        other = jnp.where(upper, pltpu.roll(x, step, 0), pltpu.roll(x, 8 - step, 0))
        return other + jnp.where(upper, -x, x)

    for k in range(2):
        gathered(*there(k)).wait_recv()

        @pl.loop(0, 8)
        def _(i):
            for j, x in enumerate(fwht([recv[k, i * 16 + j] for j in range(16)])):
                recv[k, i * 16 + j] = x

        @pl.loop(0, 16)
        def _(j):
            tiles = fwht([recv[k, i * 16 + j] for i in range(8)])
            for i in range(8):
                c, s = cosine[i, j], sine[i, j]
                if k == 0:
                    c, s = jnp.where(lower, c, pltpu.roll(c, 4, 0)), jnp.where(lower, s, -pltpu.roll(s, 4, 0))
                else:
                    c, s = jnp.where(lower, pltpu.roll(c, 4, 0), c), jnp.where(lower, pltpu.roll(s, 4, 0), -s)
                tiles[i] = tiles[i] * c + pltpu.roll(tiles[i], 4, 0) * s
            for i, x in enumerate(fwht(tiles)):
                recv[k, i * 16 + j] = x

        @pl.loop(0, 8)
        def _(i):
            tiles = fwht([recv[k, i * 16 + j] for j in range(16)])
            tiles = [turn_sublanes(turn_sublanes(x, 1), 2) for x in tiles]
            x = turn_lanes(jnp.concatenate(tiles, axis=0), signs)
            for j in range(16):
                mix[k, i * 16 + j] = x[j * 8 : j * 8 + 8]

        pair = send_to(mix.at[k], mix_in.at[k], pair_send.at[4 + k], pair_recv.at[4 + k], partner)
        pair.start()
        pair.wait()

        @pl.loop(0, 8)
        def _(i):
            for j in range(16):
                t = i * 16 + j
                back[k, t] = mix_in[k, t] + own_sign * mix[k, t]

        spread(*again(k))
        back_in[k, me] = back[k, me]

    for q in range(4):
        swap(q).wait_send()
    for d in range(7):
        send_to(level.at[0], level_mid.at[0], mid_send, mid_recv.at[0], partner).wait_send()
    level_all.wait_send()
    for k in range(2):
        gathered(*there(k)).wait_send()

    for k in range(2):
        gathered(*again(k)).wait_recv()

        @pl.loop(0, 8)
        def _(i):
            for j, x in enumerate(fwht([back_in[k, i * 16 + j] for j in range(16)])):
                out_ref[k, i * 16 + j] = x

        if k == 0:

            @pl.loop(0, 16)
            def _(j):
                for i, x in enumerate(fwht([out_ref[k, i * 16 + j] for i in range(8)])):
                    out_ref[k, i * 16 + j] = x

    for k in range(2):
        gathered(*again(k)).wait_send()


def finish(tiles_ref, out_ref, final, out_sem):
    lower = lax.broadcasted_iota(jnp.int32, (8, 128), 0) < 4
    copies = []
    for q in range(8):

        @pl.loop(q * 2, q * 2 + 2)
        def _(j):
            first, second = ([tiles_ref[k, i * 16 + j] for i in range(8)] for k in range(2))
            second = fwht(second)
            rows = pl.ds(j * 8, 8)
            for i in range(8):
                u, v = first[i] + second[i], first[i] - second[i]
                final[0, i, rows] = jnp.where(lower, u, pltpu.roll(v, 4, 0))
                final[1, i, rows] = jnp.where(lower, pltpu.roll(u, 4, 0), v)

        rows = pl.ds(q * 16, 16)
        copies.append(pltpu.make_async_copy(final.at[:, :, rows], out_ref.at[:, :, rows], out_sem.at[q]))
        copies[-1].start()
    for copy in copies:
        copy.wait()


def body(wave_parts, level_table, phase_angles):
    f32 = jnp.float32
    state, tiles = pltpu.VMEM((2, 8, 128, 128), f32), pltpu.VMEM((2, CHIPS, 8, 128), f32)
    table = pltpu.VMEM((8, 16, 8, 128), f32)
    blocks = pltpu.VMEM((8, 128, 128), f32)
    dma, regular = pltpu.SemaphoreType.DMA, pltpu.SemaphoreType.REGULAR
    anywhere, on_chip = pl.BlockSpec(memory_space=pl.ANY), pl.BlockSpec(memory_space=pltpu.VMEM)
    off_chip = pl.BlockSpec(memory_space=pltpu.HBM)
    args = [pltpu.with_memory_space_constraint(x, pltpu.HBM) for x in (wave_parts, level_table, phase_angles)]
    mixed = pl.pallas_call(
        kernel,
        out_shape=pltpu.VMEM((2, CHIPS, 8, 128), f32),
        in_specs=[off_chip] * 3,
        out_specs=on_chip,
        scratch_shapes=[
            state, blocks, pltpu.VMEM((2, 128), f32), table, table, state, state, tiles, tiles, blocks, table, tiles, tiles, tiles, tiles,
            dma((3,)), dma((6,)), dma((6,)), dma, dma((7,)), dma, dma, dma((2,)), dma((2,)), dma((2,)), dma((2,)), regular, regular((3,)), regular((3,)),
        ],
        compiler_params=pltpu.CompilerParams(collective_id=0, has_side_effects=True, vmem_limit_bytes=32 * 2**20),
    )(*args)
    return pl.pallas_call(
        finish,
        out_shape=jax.ShapeDtypeStruct(wave_parts.shape, f32),
        in_specs=[on_chip],
        out_specs=anywhere,
        scratch_shapes=[state, dma((8,))],
        compiler_params=pltpu.CompilerParams(vmem_limit_bytes=16 * 2**20),
    )(mixed)


def solution(mesh):
    in_specs = (P(None, ("qa", "qb"), None, None), P(("qa", "qb"), None, None), P())
    out_specs = P(None, ("qa", "qb"), None, None)
    return jax.shard_map(body, mesh=mesh, in_specs=in_specs, out_specs=out_specs, check_vma=False)
```
